32 devices in a mesh: ord: 8 (over z, y), blk: 4 (over x, core).
Axes of the slice: x: 2, y: 2, z: 4, core: 2. Of those that a mesh axis runs over, the one named last changes fastest.
Arguments:
- panel: bfloat16 [2880, 64, 2880], P('ord', 'blk'), as said below
- gauss: bfloat16 [2, 16, 2880, 2880], P(None, None, 'ord', 'blk'), may hold values from -2.3841858e-06 to 2.3841858e-06
- height: float32 [16], replicated, may hold values from 0.25 to 2.5
- order_map: int32 [2880], replicated, may hold values from 0 to 2879, as said below
- cycle_map: int32 [64], P('blk'), may hold values from 360 to 2519, as said below
Outputs:
- field: bfloat16 [5760, 3072], P('ord', 'blk')
The draws below stay inside these ranges and needn't reach their ends.
Inputs may be any that keep to these rules, and one draw needn't show every extreme that they name: `order_map`: a permutation of 0 to 2879; the 360 slots of each index of ord hold consecutive orders in ascending order. `panel`: entries at degrees below the order of their slot are zero. `cycle_map`: distinct cycle numbers.
All inputs are finite; a program needn't handle non-finite values.
Results may differ from the reference program's by a relative error of at most 0.0068.
Values may be sent and summed in bfloat16 or wider, within the bound.
A program may use at most 256 MiB of HBM per device.

```python
import math
import jax
import jax.numpy as jnp
from jax import lax

ORDERS = 2880
SHELLS = 16
CYCLES = 64
ORD_DEV = 360
NLON = 5760


def order_runs(key):
    runs = ORDERS // ORD_DEV
    shuffled = jax.random.permutation(key, runs).astype(jnp.int32)
    slots = shuffled[:, None] * ORD_DEV + jnp.arange(ORD_DEV).astype(jnp.int32)[None, :]
    return slots.reshape(ORDERS).astype(jnp.int32)


def draw_order_map(key, part):
    return order_runs(jax.random.fold_in(key, 11))


def draw_panel(key, part):
    orders = order_runs(jax.random.fold_in(key, 11))
    sub = jax.random.fold_in(key, 12)
    values = jax.random.normal(sub, (ORDERS, CYCLES, ORDERS), jnp.float32)
    degree = jnp.arange(ORDERS).astype(jnp.int32)
    keep = degree[None, None, :] >= orders[:, None, None]
    return jnp.where(keep, values, 0.0).astype(jnp.bfloat16)


def draw_cycle_map(key, part):
    band = 3 * ORDERS // 4
    chosen = jax.random.permutation(jax.random.fold_in(key, 13), band).astype(jnp.int32)
    return (chosen[:CYCLES] + ORDERS // 8).astype(jnp.int32)


def levels(own_key, dims, pieces, smallest, largest):
    def one(dim, blocks):
        heights = jax.random.uniform(jax.random.fold_in(jax.random.fold_in(own_key, 6), dim), (blocks,), jnp.float32, smallest / len(pieces), largest / len(pieces))
        return jnp.repeat(jnp.exp(heights), dims[dim] // blocks).reshape((-1,) + (1,) * (len(dims) - dim - 1))

    factor_of = one(*pieces[0])
    for cut in pieces[1:]:
        factor_of = factor_of * one(*cut)
    return factor_of


def normal_values(stream_key, shape, scale, bound, pieces=(), kind=jnp.bfloat16):
    values = scale * jax.random.normal(stream_key, shape, jnp.float32)
    if pieces:
        values = values * levels(stream_key, shape, pieces, -0.22, 0.18)
    return jnp.clip(values, -bound, bound).astype(kind)


def setup_inputs(seed: int = 0) -> dict:
    key_list = jax.random.split(jax.random.key(seed), 6)
    panel = draw_panel(jax.random.fold_in(key_list[5], 71), 0)
    gauss = normal_values(key_list[1], (2, SHELLS, ORDERS, ORDERS), (ORDERS ** 4 // 10) ** -0.5, 2.384185791015625e-06, ((2, 8), (3, 4)))
    height = jnp.clip(jnp.exp(jax.random.uniform(key_list[2], (SHELLS,), jnp.float32, math.log(0.25), math.log(2.5))), 0.25, 2.5)
    order_map = draw_order_map(jax.random.fold_in(key_list[5], 71), 0)
    cycle_map = draw_cycle_map(jax.random.fold_in(key_list[5], 71), 0)
    return {"panel": panel, "gauss": gauss, "height": height, "order_map": order_map, "cycle_map": cycle_map}


def cycle_angles(cycle_map):
    theta = math.pi * (cycle_map.astype(jnp.float32) + 0.5) / ORDERS
    return (jnp.cos(theta), jnp.sin(theta))

def legendre_tables(current, before, degree, orders, cosine, sine):
    deg = degree[None, None, :]
    order = orders[:, None, None]
    radial = (deg + 1.0) * current
    polar = -(deg * cosine[None, :, None] * current - jnp.sqrt(jnp.maximum(deg * deg - order * order, 0.0)) * before) / sine[None, :, None]
    azimuth = order * current / sine[None, :, None]
    return jnp.stack([radial, polar, azimuth], 2).astype(jnp.bfloat16)

def weighted(coef, degree, height):
    radial = jnp.exp(-(degree[None, :] + 2.0) * height[:, None] / ORDERS)
    return (coef.astype(jnp.float32) * radial[None, :, None, :]).astype(jnp.bfloat16)

def assemble(total, cycles, shells):
    count = total.shape[1]
    parts = total.reshape(2, count, cycles, 3, shells)
    g_part = parts[0]
    h_part = parts[1]
    cosine_part = jnp.concatenate([g_part[:, :, :2], -h_part[:, :, 2:]], 2)
    sine_part = jnp.concatenate([h_part[:, :, :2], g_part[:, :, 2:]], 2)
    return jnp.stack([cosine_part, sine_part]).reshape(2, count, cycles * 3 * shells).astype(jnp.bfloat16)

def fourier_tables(order_map, position):
    phase = order_map.astype(jnp.int32)[:, None] * position.astype(jnp.int32)[None, :] % NLON
    angle = phase.astype(jnp.float32) * (2.0 * math.pi / NLON)
    return jnp.stack([jnp.cos(angle), jnp.sin(angle)]).astype(jnp.bfloat16)

def reference(panel, gauss, height, order_map, cycle_map):
    cosine, sine = cycle_angles(cycle_map)
    degree = jnp.arange(ORDERS).astype(jnp.float32)

    def one_slot(slot):
        slot = slot.astype(jnp.int32)
        current = lax.dynamic_slice_in_dim(panel, slot, 1, 0).astype(jnp.float32)
        before = jnp.concatenate([jnp.zeros((1, CYCLES, 1), jnp.float32), current[:, :, :-1]], 2)
        order = lax.dynamic_slice_in_dim(order_map, slot, 1, 0).astype(jnp.float32)
        tables = legendre_tables(current, before, degree, order, cosine, sine).reshape(1, CYCLES * 3, ORDERS)
        coef = lax.dynamic_slice_in_dim(gauss, slot, 1, 2)
        weights = weighted(coef, degree, height)
        total = jnp.einsum('okl,gsol->goks', tables.astype(jnp.float32), weights.astype(jnp.float32))
        return assemble(total, CYCLES, SHELLS)[:, 0]
    spectra = lax.map(one_slot, jnp.arange(ORDERS).astype(jnp.int32))
    spectra = jnp.transpose(spectra, (1, 0, 2))
    tables = fourier_tables(order_map, jnp.arange(NLON).astype(jnp.int32))
    field = lax.dot_general(tables.astype(jnp.float32), spectra.astype(jnp.float32), (((0, 1), (0, 1)), ((), ())), precision=lax.Precision.HIGHEST)
    return field.astype(jnp.bfloat16)
```

```python
import math

import jax
import jax.numpy as jnp
from jax import lax
from jax.sharding import PartitionSpec as P

ORDERS = 2880
TILE = 320
NLON = 5760
GROUPS = 3


def cycle_angles(cycle_map):
    theta = math.pi * (cycle_map.astype(jnp.float32) + 0.5) / ORDERS
    return (jnp.cos(theta), jnp.sin(theta))


def legendre_tables(current, before, degree, orders, cosine, sine):
    deg = degree[None, None, :]
    order = orders[:, None, None]
    radial = (deg + 1.0) * current
    polar = (
        -(
            deg * cosine[None, :, None] * current
            - jnp.sqrt(jnp.maximum(deg * deg - order * order, 0.0)) * before
        )
        / sine[None, :, None]
    )
    azimuth = order * current / sine[None, :, None]
    return jnp.stack([radial, polar, azimuth], 2).astype(jnp.bfloat16)


def weighted(coef, degree, height):
    radial = jnp.exp(-(degree[None, :] + 2.0) * height[:, None] / ORDERS)
    return (coef.astype(jnp.float32) * radial[None, :, None, :]).astype(jnp.bfloat16)


def assemble(total, cycles, shells):
    count = total.shape[1]
    parts = total.reshape(2, count, cycles, 3, shells)
    g_part = parts[0]
    h_part = parts[1]
    cosine_part = jnp.concatenate([g_part[:, :, :2], -h_part[:, :, 2:]], 2)
    sine_part = jnp.concatenate([h_part[:, :, :2], g_part[:, :, 2:]], 2)
    return (
        jnp.stack([cosine_part, sine_part])
        .reshape(2, count, cycles * 3 * shells)
        .astype(jnp.bfloat16)
    )


def turn(steps, period):
    angle = (steps % period).astype(jnp.float32) * (2.0 * math.pi / period)
    return (jnp.cos(angle), jnp.sin(angle))


def synthesis(spread, order_map, ranks):
    items = spread.shape[2]
    count = spread.shape[1] // ranks
    period = NLON // count
    rows = NLON // period
    block = order_map.reshape(ranks, count)[:, 0] // count
    p = jnp.arange(period, dtype=jnp.int32)
    q = jnp.arange(rows, dtype=jnp.int32)
    r = jnp.arange(count, dtype=jnp.int32)
    block_cos, block_sin = turn(p[:, None] * block[None, :], period)
    mix = jnp.stack(
        [jnp.stack([block_cos, block_sin], 1), jnp.stack([-block_sin, block_cos], 1)], 1
    )
    parts = spread.reshape(2, ranks, count, items)
    mixed = jnp.einsum(
        "pckd,kdri->pcri", mix, parts.astype(jnp.float32), precision=lax.Precision.HIGHEST
    ).astype(jnp.bfloat16)
    p_cos, p_sin = turn(p[:, None] * r[None, :], NLON)
    q_cos, q_sin = turn(r[:, None] * q[None, :] * period, NLON)
    p_cos, p_sin = p_cos[:, :, None], p_sin[:, :, None]
    tables = jnp.stack([p_cos * q_cos - p_sin * q_sin, p_sin * q_cos + p_cos * q_sin], 1)
    field = jnp.einsum(
        "pcrq,pcri->pqi", tables.astype(jnp.bfloat16), mixed, preferred_element_type=jnp.float32
    )
    return field.astype(jnp.bfloat16).transpose(1, 0, 2).reshape(NLON, items)


def degree_sums(panel_src, edge, coef_src, orders, cosine, sine, height, base, first, last):
    count, cycles, _ = panel_src.shape
    shells = height.shape[0]

    def step(tile, total):
        offset = (tile * TILE - base).astype(jnp.int32)
        current = lax.dynamic_slice_in_dim(panel_src, offset, TILE, 2).astype(jnp.float32)
        earlier = lax.dynamic_slice_in_dim(panel_src, jnp.maximum(offset - 1, 0), TILE, 2).astype(
            jnp.float32
        )
        shifted = jnp.concatenate([edge[:, :, None].astype(jnp.float32), current[:, :, :-1]], 2)
        before = jnp.where(offset > 0, earlier, shifted)
        degree = (tile * TILE + jnp.arange(TILE)).astype(jnp.float32)
        tables = legendre_tables(current, before, degree, orders, cosine, sine).reshape(
            count, cycles * 3, TILE
        )
        weights = weighted(lax.dynamic_slice_in_dim(coef_src, offset, TILE, 3), degree, height)
        return total + jnp.einsum(
            "okl,gsol->goks", tables, weights, preferred_element_type=jnp.float32
        )

    init = jnp.zeros((2, count, cycles * 3, shells), jnp.float32)
    return lax.fori_loop(jnp.asarray(first, jnp.int32), jnp.asarray(last, jnp.int32), step, init)


def body(panel, gauss, height, order_map, cycle_map):
    count, cycles, degrees = panel.shape
    shells = height.shape[0]
    tiles = degrees // TILE
    cosine, sine = cycle_angles(cycle_map)
    here = lax.axis_index("ord")
    orders_int = lax.dynamic_slice_in_dim(order_map, here * count, count, 0)
    orders = orders_int.astype(jnp.float32)
    groups = GROUPS if count % GROUPS == 0 else 1
    size = count // groups
    zero_edge = jnp.zeros((size, cycles), jnp.bfloat16)
    totals = []
    for group in range(groups):
        part = slice(group * size, (group + 1) * size)
        coef = lax.all_gather(gauss[:, :, part], "blk", axis=3, tiled=True)
        totals.append(
            degree_sums(
                panel[part], zero_edge, coef, orders[part], cosine, sine, height, 0, 0, tiles
            )
        )
    total = jnp.concatenate(totals, 1)
    spectra = assemble(total, cycles, shells)
    spread = lax.all_to_all(spectra, "ord", split_axis=2, concat_axis=1, tiled=True)
    field = synthesis(spread, order_map, order_map.shape[0] // count)
    return lax.all_to_all(field, "ord", split_axis=0, concat_axis=1, tiled=True)


def solution(mesh):
    return jax.shard_map(
        body,
        mesh=mesh,
        in_specs=(P("ord", "blk", None), P(None, None, "ord", "blk"), P(), P(), P("blk")),
        out_specs=P("ord", "blk"),
        check_vma=False,
    )
```
